32 devices in a mesh: dp: 1 (over z), tp: 32 (over y, x, core).
Axes of the slice: x: 4, y: 4, z: 1, core: 2. Of those that a mesh axis runs over, the one named last changes fastest.
The devices are a block of a 4x4x8 slice.
Arguments:
- hidden: bfloat16 [8192, 4096], P(('dp', 'tp'))
- ln_gain: float32 [4096], replicated
- ln_bias: float32 [4096], replicated
- out_embed: bfloat16 [32768, 4096], P('tp')
- vocab_valid: int32 [32768], P('tp')
- targets: int32 [8192], P(('dp', 'tp'))
- loss_mask: int32 [8192], P(('dp', 'tp'))
Outputs:
- output 1: float32 [8192], P(('dp', 'tp'))
- output 2: float32 [1], P('dp')
- output 3: bfloat16 [8192, 4096], P(('dp', 'tp'))
- output 4: float32 [32768, 4096], P(('dp', 'tp'))
- output 5: float32 [4096], P('dp')
- output 6: float32 [4096], P('dp')
All inputs are finite; a program needn't handle non-finite values.
Results may differ from the reference program's by a relative error of at most 0.001.
Values are sent between devices in bfloat16 or wider.
A program may use at most 768 MiB of HBM per device.

```python
import jax
import jax.numpy as jnp
from jax import lax

MODEL_DIM = 4096
VOCAB_REAL = 32768
VOCAB_PAD = 32768
SEQ_LEN = 8192
TOK_BLOCK = 256
BLOCK_COUNT = SEQ_LEN // TOK_BLOCK
SOFT_CAP = 30.0
Z_COEF = 1e-4
LN_EPS = 1e-5


def layer_norm(h_float, ln_gain, ln_bias):
    mean_val = jnp.mean(h_float, axis=-1, keepdims=True)
    centered = h_float - mean_val
    var_val = jnp.mean(centered * centered, axis=-1, keepdims=True)
    return centered * lax.rsqrt(var_val + LN_EPS) * ln_gain + ln_bias


def draw_layout(shared_key, part_key):
    col_idx = jnp.arange(VOCAB_PAD)
    coin_draw = jax.random.randint(shared_key, (VOCAB_PAD,), 0, 8)
    dropped = (col_idx % 2 == 0) & (coin_draw == 0) & (col_idx < VOCAB_REAL - 1)
    vocab_valid = ((col_idx < VOCAB_REAL) & jnp.logical_not(dropped)).astype(jnp.int32)
    key_tgt, key_pre, key_post, key_hole = jax.random.split(part_key, 4)
    raw_tgt = jax.random.randint(key_tgt, (SEQ_LEN,), 0, VOCAB_REAL)
    targets = raw_tgt + 1 - vocab_valid[raw_tgt]
    positions = jnp.arange(SEQ_LEN)
    prefix_len = jax.random.randint(key_pre, (), 0, SEQ_LEN // 4 + 1)
    suffix_len = jax.random.randint(key_post, (), 0, SEQ_LEN // 4 + 1)
    hole_draw = jax.random.randint(key_hole, (SEQ_LEN,), 0, 8)
    keep_tok = (positions >= prefix_len) & (positions < SEQ_LEN - suffix_len) & (hole_draw != 0)
    keep_tok = keep_tok | (positions == SEQ_LEN // 2)
    return vocab_valid, targets.astype(jnp.int32), keep_tok.astype(jnp.int32)


def setup_inputs(seed: int = 0, part: int = 0) -> dict:
    shared_key = jax.random.key(seed)
    part_key = jax.random.fold_in(jax.random.key(seed + 1), part)
    key_gain, key_bias, key_embed, key_valid = jax.random.split(shared_key, 4)
    key_hidden, key_layout = jax.random.split(part_key, 2)
    hidden = 1.5 * jax.random.normal(key_hidden, (SEQ_LEN, MODEL_DIM), jnp.float32)
    ln_gain = 1.0 + 0.3 * jax.random.normal(key_gain, (MODEL_DIM,), jnp.float32)
    ln_bias = 0.3 * jax.random.normal(key_bias, (MODEL_DIM,), jnp.float32)
    out_embed = (3.0 * MODEL_DIM ** -0.5) * jax.random.normal(key_embed, (VOCAB_PAD, MODEL_DIM), jnp.float32)
    vocab_valid, targets, loss_mask = draw_layout(key_valid, key_layout)
    return {"hidden": hidden.astype(jnp.bfloat16), "ln_gain": ln_gain, "ln_bias": ln_bias, "out_embed": out_embed.astype(jnp.bfloat16), "vocab_valid": vocab_valid, "targets": targets, "loss_mask": loss_mask}


def reference(hidden, ln_gain, ln_bias, out_embed, vocab_valid, targets, loss_mask):
    normed, ln_back = jax.vjp(layer_norm, hidden.astype(jnp.float32), ln_gain, ln_bias)
    x_all = normed.astype(jnp.bfloat16)
    mask_f = loss_mask.astype(jnp.float32)
    tok_count = jnp.sum(mask_f)
    col_ok = (vocab_valid != 0)[None, :]
    col_ids = jnp.arange(VOCAB_PAD)[None, :]

    def block_step(embed_grad, blk_data):
        x_blk, tgt_blk, mask_blk = blk_data
        logits = jnp.dot(x_blk, out_embed.T, preferred_element_type=jnp.float32)
        tanh_val = jnp.tanh(logits / SOFT_CAP)
        capped = SOFT_CAP * tanh_val
        masked = jnp.where(col_ok, capped, -SOFT_CAP)
        row_max = jnp.max(masked, axis=1, keepdims=True)
        exp_vals = jnp.where(col_ok, jnp.exp(masked - row_max), 0.0)
        sum_exp = jnp.sum(exp_vals, axis=1, keepdims=True)
        lse = row_max[:, 0] + jnp.log(sum_exp[:, 0])
        is_target = tgt_blk[:, None] == col_ids
        tgt_logit = jnp.sum(jnp.where(is_target, capped, 0.0), axis=1)
        tok_loss = (lse - tgt_logit + Z_COEF * lse * lse) * mask_blk
        tok_coef = mask_blk / tok_count
        d_capped = ((1.0 + 2.0 * Z_COEF * lse) * tok_coef)[:, None] * (exp_vals / sum_exp) - jnp.where(is_target, tok_coef[:, None], 0.0)
        d_logits = (d_capped * (1.0 - tanh_val * tanh_val)).astype(jnp.bfloat16)
        new_grad = embed_grad + jnp.dot(d_logits.T, x_blk, preferred_element_type=jnp.float32)
        d_normed = jnp.dot(d_logits, out_embed, preferred_element_type=jnp.float32)
        return new_grad, (tok_loss, d_normed)

    init_grad = jnp.zeros((VOCAB_PAD, MODEL_DIM), jnp.float32)
    blk_inputs = (x_all.reshape(BLOCK_COUNT, TOK_BLOCK, MODEL_DIM), targets.reshape(BLOCK_COUNT, TOK_BLOCK), mask_f.reshape(BLOCK_COUNT, TOK_BLOCK))
    d_embed, (tok_loss, d_normed) = lax.scan(block_step, init_grad, blk_inputs)
    tok_loss = tok_loss.reshape(SEQ_LEN)
    d_normed = d_normed.reshape(SEQ_LEN, MODEL_DIM)
    mean_loss = jnp.sum(tok_loss) / tok_count
    d_hidden, d_gain, d_bias = ln_back(d_normed)
    return tok_loss, mean_loss.reshape(1), d_hidden.astype(jnp.bfloat16), d_embed, d_gain, d_bias
```

```python
import functools
import math

import jax
import jax.numpy as jnp
from jax import lax
from jax.experimental import pallas as pl
from jax.experimental.pallas import tpu as pltpu
from jax.sharding import PartitionSpec as P

SOFT_CAP = 30.0
Z_COEF = 1e-4
LN_EPS = 1e-5

RINGS = 4
MESH = pl.DeviceIdType.MESH
F32 = jnp.float32
BF16 = jnp.bfloat16
HBM = pl.BlockSpec(memory_space=pltpu.HBM)
DMA = pltpu.SemaphoreType.DMA
VMEM_LIMIT = 66_000_000


def layer_norm(h_float, ln_gain, ln_bias):
    mean_val = jnp.mean(h_float, axis=-1, keepdims=True)
    centered = h_float - mean_val
    var_val = jnp.mean(centered * centered, axis=-1, keepdims=True)
    return centered * lax.rsqrt(var_val + LN_EPS) * ln_gain + ln_bias


class Place:
    def __init__(self, n):
        self.chips = n // 2
        self.side = math.isqrt(self.chips)
        idx = lax.axis_index("tp")
        self.idx = idx
        self.core = lax.rem(idx, 2)
        self.chip = idx // 2
        x = lax.rem(self.chip, self.side)
        y = self.chip // self.side
        d = lax.rem(x + y, self.side)
        self.pos = [self.side * y + d, self.side * x + d]
        self.partner = idx + 1 - 2 * self.core

    def chip_at(self, q, p):
        p = lax.rem(p + 2 * self.chips, self.chips)
        major = p // self.side
        minor = lax.rem(lax.rem(p, self.side) - major + self.side, self.side)
        return major * self.side + minor if q < 2 else minor * self.side + major

    def step(self, q, s):
        return self.chip_at(q, self.pos[q // 2] - s if q % 2 == 0 else self.pos[q // 2] + s)

    def ring_next(self, q):
        return self.step(q, -1) * 2 + self.core

    def ring_prev(self, q):
        return self.step(q, 1) * 2 + self.core

    def peer(self, d):
        return lax.rem(self.chip + d, self.chips) * 2 + self.core


def to(device):
    return dict(device_id={"tp": device}, device_id_type=MESH)


def meet(at):
    bar = pltpu.get_barrier_semaphore()

    def hello(d, _):
        pl.semaphore_signal(bar, inc=1, **to(at.peer(d)))
        return 0

    lax.fori_loop(1, at.chips, hello, 0)
    pl.semaphore_signal(bar, inc=1, **to(at.partner))
    pl.semaphore_wait(bar, at.chips)


def ring_lane(width, sub):
    lane = lax.broadcasted_iota(jnp.int32, (1, width), 1)
    return lax.rem(lane // sub, RINGS)


def pick(at, table, s, lane_ring):
    row = lax.broadcasted_iota(jnp.int32, table.shape, 0)
    owner = at.step(0, s)
    for q in range(1, RINGS):
        owner = jnp.where(lane_ring == q, at.step(q, s), owner)
    return jnp.sum(jnp.where(row == owner, table, jnp.zeros_like(table)), axis=0, keepdims=True)


def gather_kernel(n, x_ref, e_ref, vv_ref, meta_ref, g_ref, t_ref, ep_ref, vvp_ref, metas_ref, stats_ref,
                  emb, valid, tile, stage, metas, st,
                  send, recv, msend, mrecv, psend, precv, esem, lsem, tsem, osem):
    at = Place(n)
    chips = at.chips
    rows = x_ref.shape[0]
    half = rows // 2
    sub = half // RINGS
    voc = e_ref.shape[0]
    rb = stage.shape[1]
    blocks = 2 * voc // rb

    def ring(src, s, q, h):
        part = pl.ds(h * half + q * sub, sub)
        return pltpu.make_async_remote_copy(
            src_ref=src.at[part], dst_ref=g_ref.at[s + 1, part],
            send_sem=send.at[s, q, h], recv_sem=recv.at[s, q, h], **to(at.ring_next(q)))

    def load(s, h):
        part = pl.ds(h * half, half)
        return pltpu.make_async_copy(g_ref.at[s, part], tile.at[lax.rem(s, 2), part], lsem.at[lax.rem(s, 2), h])

    def tell(d):
        return pltpu.make_async_remote_copy(
            src_ref=meta_ref, dst_ref=metas.at[at.chip], send_sem=msend.at[d], recv_sem=mrecv.at[d], **to(at.peer(d)))

    own = pltpu.make_async_copy(e_ref, emb.at[pl.ds(0, voc)], esem.at[0])
    own_valid = pltpu.make_async_copy(vv_ref, valid.at[pl.ds(0, voc)], esem.at[1])
    own_meta = pltpu.make_async_copy(meta_ref, metas.at[at.chip], esem.at[2])
    own_x = [pltpu.make_async_copy(x_ref.at[pl.ds(h * half, half)], tile.at[0, pl.ds(h * half, half)], lsem.at[0, h])
             for h in range(2)]
    give = pltpu.make_async_remote_copy(
        src_ref=e_ref, dst_ref=emb.at[pl.ds(voc, voc)], send_sem=psend.at[0], recv_sem=precv.at[0], **to(at.partner))
    give_valid = pltpu.make_async_remote_copy(
        src_ref=vv_ref, dst_ref=valid.at[pl.ds(voc, voc)], send_sem=psend.at[1], recv_sem=precv.at[1], **to(at.partner))

    own.start()
    own_valid.start()
    own_meta.start()
    for c in own_x:
        c.start()
    meet(at)
    for h in range(2):
        for q in range(RINGS):
            ring(x_ref, 0, q, h).start()

    def tell_all(d, _):
        tell(d).start()
        return 0

    lax.fori_loop(1, chips, tell_all, 0)
    give.start()
    give_valid.start()
    st[...] = jnp.zeros_like(st)

    def hear(d, _):
        tell(d).wait_recv()
        return 0

    own_meta.wait()
    lax.fori_loop(1, chips, hear, 0)
    own.wait()
    own_valid.wait()

    lane_ring = ring_lane(rows, sub)
    row_id = lax.broadcasted_iota(jnp.int32, (rb, 1), 0)
    base = [at.idx * voc, at.partner * voc]
    table_row = lax.broadcasted_iota(jnp.int32, (chips, rows), 0)

    def put(s, b):
        return pltpu.make_async_copy(stage.at[b % 4], t_ref.at[s, pl.ds(b * rb, rb)], tsem.at[b % 4])

    def step(s, _):
        slot = lax.rem(s, 2)
        tgt = pick(at, metas[:, 0, :], s, lane_ring)
        for h in range(2):
            pltpu.make_async_copy(x_ref.at[pl.ds(0, half)], tile.at[slot, pl.ds(h * half, half)], lsem.at[slot, h]).wait()

        keep = pltpu.make_async_copy(tile.at[0], g_ref.at[0], osem.at[2])

        @pl.when(s == 0)
        def _():
            keep.start()

        def arrive(h):
            @pl.when(s < chips - 1)
            def _():
                for q in range(RINGS):
                    ring(x_ref, s, q, h).wait_recv()

                    @pl.when(s < chips - 2)
                    def _():
                        ring(g_ref.at[s + 1], s + 1, q, h).start()
                load(s + 1, h).start()

        sums = jnp.zeros((1, rows), F32)
        hits = jnp.zeros((1, rows), F32)
        for b in range(blocks):
            if b == 0:
                arrive(0)
            if b == blocks - 1:
                arrive(1)
            if b == blocks // 2:
                @pl.when(s == 0)
                def _():
                    give.wait_recv()
                    give_valid.wait_recv()
                    pltpu.make_async_copy(emb.at[pl.ds(voc, voc)], ep_ref, osem.at[0]).start()
                    pltpu.make_async_copy(valid.at[pl.ds(voc, voc)], vvp_ref, osem.at[1]).start()
            z = lax.dot_general(emb[pl.ds(b * rb, rb), :], tile[slot], (((1,), (1,)), ((), ())),
                                preferred_element_type=F32)
            t = jnp.tanh(z * (1.0 / SOFT_CAP))
            @pl.when(s > 0)
            def _():
                put(s, b).wait()
            stage[b % 4] = t
            put(s, b).start()
            capped = SOFT_CAP * t
            ok = valid[pl.ds(b * rb, rb), :]
            ex = jnp.exp(capped) * jnp.concatenate([ok] * (rows // ok.shape[1]), axis=1)
            sums += jnp.sum(ex, axis=0, keepdims=True)
            first = base[(b * rb) // voc] + (b * rb) % voc
            hits += jnp.sum(jnp.where(row_id + first == tgt, capped, 0.0), axis=0, keepdims=True)
        owner = at.step(0, s)
        for q in range(1, RINGS):
            owner = jnp.where(lane_ring == q, at.step(q, s), owner)
        mine = table_row == owner

        @pl.when(s == 0)
        def _():
            keep.wait()
        st[0] = jnp.where(mine, sums, st[0])
        st[1] = jnp.where(mine, hits, st[1])
        return 0

    lax.fori_loop(0, chips, step, 0)
    outs = [pltpu.make_async_copy(metas, metas_ref, osem.at[2]), pltpu.make_async_copy(st, stats_ref, osem.at[3])]
    for c in outs:
        c.start()

    def drain(s, _):
        for h in range(2):
            for q in range(RINGS):
                ring(x_ref, s, q, h).wait_send()
        return 0

    lax.fori_loop(0, chips - 1, drain, 0)

    def told(d, _):
        tell(d).wait_send()
        return 0

    lax.fori_loop(1, chips, told, 0)
    give.wait_send()
    give_valid.wait_send()
    for b in range(blocks):
        put(0, b).wait()
    pltpu.make_async_copy(emb.at[pl.ds(voc, voc)], ep_ref, osem.at[0]).wait()
    pltpu.make_async_copy(valid.at[pl.ds(voc, voc)], vvp_ref, osem.at[1]).wait()
    for c in outs:
        c.wait()


def gather(n, x, e, vv, meta):
    chips = n // 2
    rows, dim = x.shape
    voc = e.shape[0]
    rb = voc // 2
    blocks = 2 * voc // rb
    shapes = (
        jax.ShapeDtypeStruct((chips, rows, dim), BF16),
        jax.ShapeDtypeStruct((chips, 2 * voc, rows), F32),
        jax.ShapeDtypeStruct((voc, dim), BF16),
        jax.ShapeDtypeStruct(vv.shape, F32),
        jax.ShapeDtypeStruct((chips,) + meta.shape, jnp.int32),
        jax.ShapeDtypeStruct((2, chips, rows), F32),
    )
    flops = 2 * chips * rows * 2 * voc * dim
    return pl.pallas_call(
        functools.partial(gather_kernel, n),
        out_shape=shapes,
        in_specs=[HBM] * 4,
        out_specs=(HBM,) * len(shapes),
        scratch_shapes=[
            pltpu.VMEM((2 * voc, dim), BF16),
            pltpu.VMEM((2 * voc, vv.shape[1]), F32),
            pltpu.VMEM((2, rows, dim), BF16),
            pltpu.VMEM((4, rb, rows), F32),
            pltpu.VMEM((chips,) + meta.shape, jnp.int32),
            pltpu.VMEM((2, chips, rows), F32),
            DMA((chips, RINGS, 2)), DMA((chips, RINGS, 2)),
            DMA((chips,)), DMA((chips,)),
            DMA((2,)), DMA((2,)),
            DMA((3,)), DMA((2, 2)), DMA((4,)), DMA((4,)),
        ],
        compiler_params=pltpu.CompilerParams(collective_id=0, has_side_effects=True, vmem_limit_bytes=VMEM_LIMIT),
        cost_estimate=pl.CostEstimate(flops=flops, bytes_accessed=0, transcendentals=0),
        name="gather_logits",
    )(x, e, vv, meta)


def scatter_kernel(n, g_ref, t_ref, e_ref, ep_ref, vv_ref, vvp_ref, metas_ref, stats_ref,
                   dx_ref, de_ref, loss_ref,
                   emb, dzt, acc, land, stage, xcol, de_own, de_send, de_land, dzn, valid, stat_all, metas, coef, cnt, lossv,
                   send, recv, credit, ssend, srecv, csem, lsem, zsem, xsem, psend, precv, pcredit, osem, nsend, nrecv):
    at = Place(n)
    chips = at.chips
    rows, dim = dx_ref.shape
    half = rows // 2
    sub = half // RINGS
    voc = e_ref.shape[0]
    rb = stage.shape[1]
    blocks = 2 * voc // rb
    cols = xcol.shape[1]
    col_blocks = dim // cols
    units = 2 * chips

    def ring(k, q, h):
        src = pl.ds(pl.multiple_of(q * sub, sub), sub)
        return pltpu.make_async_remote_copy(
            src_ref=acc.at[h, lax.rem(k, 2), src], dst_ref=land.at[h, lax.rem(k, 2), src],
            send_sem=send.at[k, q, h], recv_sem=recv.at[k, q, h], **to(at.ring_next(q)))

    def share(d):
        return pltpu.make_async_remote_copy(
            src_ref=stats_ref, dst_ref=stat_all.at[at.chip], send_sem=ssend.at[d], recv_sem=srecv.at[d], **to(at.peer(d)))

    loads = [
        pltpu.make_async_copy(metas_ref, metas, lsem.at[0]),
        pltpu.make_async_copy(stats_ref, stat_all.at[at.chip], lsem.at[1]),
        pltpu.make_async_copy(vv_ref, valid.at[pl.ds(0, voc)], lsem.at[2]),
        pltpu.make_async_copy(vvp_ref, valid.at[pl.ds(voc, voc)], lsem.at[3]),
        pltpu.make_async_copy(e_ref, emb.at[pl.ds(0, voc)], lsem.at[4]),
        pltpu.make_async_copy(ep_ref, emb.at[pl.ds(voc, voc)], lsem.at[5]),
    ]
    for c in loads:
        c.start()

    def zload(o, b):
        return pltpu.make_async_copy(t_ref.at[lax.rem(o + 1, chips), pl.ds(b * rb, rb)], stage.at[b % 2], zsem.at[b % 2])

    zload(0, 0).start()
    meet(at)

    def share_all(d, _):
        share(d).start()
        return 0

    lax.fori_loop(1, chips, share_all, 0)

    loads[0].wait()
    mask = metas[:, 1, :].astype(F32)
    cnt[0] = jnp.full(cnt.shape[1:], jnp.sum(mask), F32)
    swap = pltpu.make_async_remote_copy(src_ref=cnt.at[0], dst_ref=cnt.at[1], send_sem=nsend, recv_sem=nrecv, **to(at.partner))
    swap.start()

    def hear(d, _):
        share(d).wait_recv()
        return 0

    loads[1].wait()
    lax.fori_loop(1, chips, hear, 0)
    swap.wait()
    total = cnt[0, 0:1, 0:1] + cnt[1, 0:1, 0:1]
    sum_exp = jnp.sum(stat_all[:, 0], axis=0)
    hits = jnp.sum(stat_all[:, 1], axis=0)
    lse = jnp.log(sum_exp)
    tok_coef = mask / total
    coef[0] = (1.0 + 2.0 * Z_COEF * lse) * tok_coef / sum_exp
    coef[1] = tok_coef
    loss = (lse - hits + Z_COEF * lse * lse) * mask
    table_row = lax.broadcasted_iota(jnp.int32, loss.shape, 0)
    own_loss = jnp.sum(jnp.where(table_row == at.chip, loss, 0.0), axis=0, keepdims=True)
    out_row = lax.broadcasted_iota(jnp.int32, lossv.shape, 0)
    lossv[...] = jnp.where(out_row == 0, own_loss, jnp.sum(own_loss) / total)
    out_loss = pltpu.make_async_copy(lossv, loss_ref, osem.at[2])
    out_loss.start()

    lane_ring = ring_lane(rows, sub)
    row_id = lax.broadcasted_iota(jnp.int32, (rb, 1), 0)
    base = [at.idx * voc, at.partner * voc]

    def d_logits(o):
        s = lax.rem(o + 1, chips)
        tgt = pick(at, metas[:, 0, :], s, lane_ring)
        ca = pick(at, coef[0], s, lane_ring)
        cb = pick(at, coef[1], s, lane_ring)
        lanes = pl.ds(pl.multiple_of(s * rows, rows), rows)
        for b in range(blocks):
            zload(o, b).wait()
            if b + 1 < blocks:
                zload(o, b + 1).start()
            else:
                @pl.when(o + 1 < chips)
                def _():
                    zload(o + 1, 0).start()
            t = stage[b % 2]
            ok = valid[pl.ds(b * rb, rb), :]
            ex = jnp.exp(SOFT_CAP * t) * jnp.concatenate([ok] * (rows // ok.shape[1]), axis=1)
            first = base[(b * rb) // voc] + (b * rb) % voc
            d_cap = ca * ex - jnp.where(row_id + first == tgt, cb, 0.0)
            dzt[pl.ds(b * rb, rb), lanes] = (d_cap * (1.0 - t * t)).astype(BF16)

    nb = 512

    def d_x(k, h):
        s = lax.rem(k, chips)
        lanes = pl.ds(pl.multiple_of(s * rows + h * half, half), half)
        for r in range(2 * voc // half):
            dzn[:, pl.ds(r * half, half)] = dzt[pl.ds(r * half, half), lanes].T

        def block(j, _):
            c = pl.ds(pl.multiple_of(j * nb, nb), nb)
            acc[h, lax.rem(k, 2), :, c] = jnp.dot(dzn[...], emb[:, c], preferred_element_type=F32)
            return 0

        lax.fori_loop(0, dim // nb, block, 0)

    def xload(b):
        return pltpu.make_async_copy(g_ref.at[:, pl.ds(pl.multiple_of(b * cols, cols), cols)], xcol, xsem)

    def give(b):
        return pltpu.make_async_remote_copy(src_ref=de_send, dst_ref=de_land, send_sem=psend, recv_sem=precv, **to(at.partner))

    def out_de(b):
        return pltpu.make_async_copy(de_own.at[lax.rem(b, 2)],
                                     de_ref.at[:, pl.ds(pl.multiple_of(b * cols, cols), cols)], osem.at[lax.rem(b, 2)])

    rc = 512

    def de_finish(b):
        give(b).wait_recv()
        slot = lax.rem(b, 2)
        de_own[slot] = de_own[slot] + de_land[...]

        @pl.when(b < col_blocks - 1)
        def _():
            pl.semaphore_signal(pcredit, inc=1, **to(at.partner))
        out_de(b).start()

    def de_block(b):
        xload(b).wait()
        slot = lax.rem(b, 2)

        @pl.when(b > 0)
        def _():
            give(b).wait_send()

        def part(i, _):
            r = pl.ds(pl.multiple_of(i * rc, rc), rc)
            de_send[r] = jnp.dot(dzt[pl.ds(pl.multiple_of(voc + i * rc, rc), rc), :], xcol[...], preferred_element_type=F32)
            return 0

        lax.fori_loop(0, voc // rc, part, 0)

        @pl.when(b > 0)
        def _():
            pl.semaphore_wait(pcredit, 1)
        give(b).start()

        @pl.when(b >= 2)
        def _():
            out_de(b).wait()

        def part2(i, _):
            r = pl.ds(pl.multiple_of(i * rc, rc), rc)
            de_own[slot, r] = jnp.dot(dzt[r, :], xcol[...], preferred_element_type=F32)
            return 0

        lax.fori_loop(0, voc // rc, part2, 0)

        @pl.when(b < col_blocks - 1)
        def _():
            xload(b + 1).start()

    for c in loads[2:4]:
        c.wait()
    d_logits(0)
    for c in loads[4:]:
        c.wait()
    d_x(1, 0)
    d_x(1, 1)
    first_de = units - 1 - col_blocks

    def unit(u, _):
        k = 1 + u // 2
        h = lax.rem(u, 2)

        @pl.when(k > 1)
        def _():
            for q in range(RINGS):
                ring(k - 1, q, h).wait_recv()

            def add(i, _):
                r = pl.ds(pl.multiple_of(i * 8, 8), 8)
                acc[h, lax.rem(k, 2), r] += land[h, lax.rem(k - 1, 2), r]
                return 0

            lax.fori_loop(0, half // 8, add, 0)

            @pl.when(k < chips - 1)
            def _():
                for q in range(RINGS):
                    pl.semaphore_signal(credit.at[q, h], inc=1, **to(at.ring_prev(q)))

        @pl.when(k < chips)
        def _():
            for q in range(RINGS):
                @pl.when(k > 2)
                def _():
                    pl.semaphore_wait(credit.at[q, h], 1)
                ring(k, q, h).start()

        @pl.when(u < chips - 1)
        def _():
            d_logits(u + 1)

        @pl.when(u == first_de - 1)
        def _():
            xload(0).start()

        @pl.when(k < chips)
        def _():
            @pl.when(k > 1)
            def _():
                for q in range(RINGS):
                    ring(k - 1, q, h).wait_send()
            d_x(k + 1, h)

        @pl.when((u > first_de) & (u <= first_de + col_blocks))
        def _():
            de_finish(u - first_de - 1)

        @pl.when((u >= first_de) & (u < first_de + col_blocks))
        def _():
            de_block(u - first_de)
        return 0

    lax.fori_loop(0, units, unit, 0)
    outs = [pltpu.make_async_copy(acc.at[h, 0], dx_ref.at[pl.ds(h * half, half)], csem.at[h]) for h in range(2)]
    for c in outs:
        c.start()
    for h in range(2):
        for q in range(RINGS):
            ring(chips - 1, q, h).wait_send()

    def shared(d, _):
        share(d).wait_send()
        return 0

    lax.fori_loop(1, chips, shared, 0)
    give(0).wait_send()
    out_de(0).wait()
    out_de(1).wait()
    out_loss.wait()
    for c in outs:
        c.wait()


def scatter(n, g, t, e, ep, vv, vvp, metas, stats):
    chips, rows, dim = g.shape
    g = g.reshape(-1, dim)
    voc = e.shape[0]
    half = rows // 2
    rb, cols = 512, 256
    shapes = (
        jax.ShapeDtypeStruct((rows, dim), F32),
        jax.ShapeDtypeStruct((voc, dim), F32),
        jax.ShapeDtypeStruct((8, rows), F32),
    )
    flops = 4 * chips * rows * 2 * voc * dim
    return pl.pallas_call(
        functools.partial(scatter_kernel, n),
        out_shape=shapes,
        in_specs=[HBM] * 8,
        out_specs=(HBM,) * len(shapes),
        scratch_shapes=[
            pltpu.VMEM((2 * voc, dim), BF16),
            pltpu.VMEM((2 * voc, chips * rows), BF16),
            pltpu.VMEM((2, 2, half, dim), F32),
            pltpu.VMEM((2, 2, half, dim), F32),
            pltpu.VMEM((2, rb, rows), F32),
            pltpu.VMEM((chips * rows, cols), BF16),
            pltpu.VMEM((2, voc, cols), F32),
            pltpu.VMEM((voc, cols), F32),
            pltpu.VMEM((voc, cols), F32),
            pltpu.VMEM((half, 2 * voc), BF16),
            pltpu.VMEM((2 * voc, vv.shape[1]), F32),
            pltpu.VMEM((chips, 2, chips, rows), F32),
            pltpu.VMEM(metas.shape, jnp.int32),
            pltpu.VMEM((2, chips, rows), F32),
            pltpu.VMEM((2, 8, 128), F32),
            pltpu.VMEM((8, rows), F32),
            DMA((chips, RINGS, 2)), DMA((chips, RINGS, 2)), pltpu.SemaphoreType.REGULAR((RINGS, 2)),
            DMA((chips,)), DMA((chips,)), DMA((2,)), DMA((6,)), DMA((2,)), DMA,
            DMA, DMA, pltpu.SemaphoreType.REGULAR, DMA((3,)), DMA, DMA,
        ],
        compiler_params=pltpu.CompilerParams(collective_id=1, has_side_effects=True, vmem_limit_bytes=VMEM_LIMIT),
        cost_estimate=pl.CostEstimate(flops=flops, bytes_accessed=0, transcendentals=0),
        name="scatter_grads",
    )(g, t, e, ep, vv, vvp, metas, stats)


def total_kernel(n, p_ref, o_ref, part, pair, land, whole, psend, precv, send, recv, hsend, hrecv):
    at = Place(n)
    rows = p_ref.shape[0]
    half = rows // 2
    meet(at)
    swap = pltpu.make_async_remote_copy(src_ref=p_ref, dst_ref=pair, send_sem=psend, recv_sem=precv, **to(at.partner))
    swap.start()
    swap.wait()
    mine = pl.ds(pl.multiple_of(at.core * half, 8), half)
    part[...] = p_ref[mine] + pair[mine]
    land[at.chip] = part[...]

    def send_to(d):
        return pltpu.make_async_remote_copy(
            src_ref=part, dst_ref=land.at[at.chip], send_sem=send.at[d], recv_sem=recv.at[d], **to(at.peer(d)))

    def start(d, _):
        send_to(d).start()
        return 0

    def wait(d, _):
        send_to(d).wait()
        return 0

    lax.fori_loop(1, at.chips, start, 0)
    lax.fori_loop(1, at.chips, wait, 0)
    whole[mine] = jnp.sum(land[...], axis=0)
    back = pltpu.make_async_remote_copy(src_ref=whole.at[mine], dst_ref=whole.at[mine], send_sem=hsend, recv_sem=hrecv, **to(at.partner))
    back.start()
    back.wait()
    o_ref[...] = whole[...]


def total(n, p):
    chips = n // 2
    half = p.shape[0] // 2
    vm = pl.BlockSpec(memory_space=pltpu.VMEM)
    return pl.pallas_call(
        functools.partial(total_kernel, n),
        out_shape=jax.ShapeDtypeStruct(p.shape, F32),
        in_specs=[vm],
        out_specs=vm,
        scratch_shapes=[
            pltpu.VMEM((half, p.shape[1]), F32),
            pltpu.VMEM(p.shape, F32),
            pltpu.VMEM((chips, half, p.shape[1]), F32),
            pltpu.VMEM(p.shape, F32),
            DMA, DMA, DMA((chips,)), DMA((chips,)), DMA, DMA,
        ],
        compiler_params=pltpu.CompilerParams(collective_id=2, has_side_effects=True),
        name="small_totals",
    )(p)


def solution(mesh):
    n = mesh.shape["tp"]

    def group_step(hidden, ln_gain, ln_bias, out_embed, vocab_valid, targets, loss_mask):
        rows, dim = hidden.shape
        normed, ln_back = jax.vjp(layer_norm, hidden.astype(F32), ln_gain, ln_bias)
        x = normed.astype(BF16)
        vv = jnp.broadcast_to((vocab_valid != 0).astype(F32)[:, None], (vocab_valid.shape[0], 128))
        meta = jnp.concatenate([targets[None], loss_mask[None], jnp.zeros((6, rows), jnp.int32)], axis=0)
        g, t, ep, vvp, metas, stats = gather(n, x, out_embed, vv, meta)
        dx, d_embed, loss = scatter(n, g, t, out_embed, ep, vv, vvp, metas, stats)
        d_hidden, gain_part, bias_part = ln_back(dx)
        lanes = 128
        parts = jnp.concatenate([gain_part.reshape(-1, lanes), bias_part.reshape(-1, lanes),
                                 jnp.broadcast_to(loss[1:2, :lanes], (16, lanes))], axis=0)
        sums = total(n, parts)
        k = dim // lanes
        return (loss[0], sums[2 * k, :1], d_hidden.astype(BF16), d_embed,
                sums[:k].reshape(-1), sums[k:2 * k].reshape(-1))

    row_spec = P(("dp", "tp"))
    mat_spec = P(("dp", "tp"), None)
    return jax.shard_map(
        group_step, mesh=mesh,
        in_specs=(mat_spec, P(None), P(None), P("tp", None), P("tp"), row_spec, row_spec),
        out_specs=(row_spec, P("dp"), mat_spec, mat_spec, P("dp"), P("dp")), check_vma=False)
```
